128 devices in a mesh: fsdp: 8 (over z_hi, y), tp: 16 (over z_lo, x, core).
Axes of the slice: x: 4, y: 4, z: 4 (z_hi: 2, z_lo: 2; z = z_hi * 2 + z_lo), core: 2. Of those that a mesh axis runs over, the one named last changes fastest.
Arguments:
- tokens: bfloat16 [2048, 8192], P('fsdp', 'tp'), may hold values from -6 to 6
- out_grad: bfloat16 [2048, 8192], P('fsdp', 'tp'), may hold values from -6 to 6
- gate_weight: bfloat16 [8192, 2048], P('fsdp', 'tp'), may hold values from -0.0625 to 0.0625
- up_weight: bfloat16 [8192, 2048], P('fsdp', 'tp'), may hold values from -0.0625 to 0.0625
- down_weight: bfloat16 [2048, 8192], P('tp', 'fsdp'), may hold values from -0.125 to 0.125
Outputs:
- input_grad: bfloat16 [2048, 8192], P('fsdp', 'tp')
- gate_grad: float32 [8192, 2048], P('fsdp', 'tp')
- up_grad: float32 [8192, 2048], P('fsdp', 'tp')
- down_grad: float32 [2048, 8192], P('tp', 'fsdp')
The draws below stay inside these ranges and needn't reach their ends.
All inputs are finite; a program needn't handle non-finite values.
Results may differ from the reference program's by a relative error of at most 0.0023.
Values may be sent and summed in bfloat16 or wider, within the bound.
No kernel may reach another device: no remote copies, remote signals or barrier semaphores. Data moves between devices by JAX's collectives and lax.ppermute only.
A program may use at most 128 MiB of HBM per device.

```python
import math
import jax
import jax.numpy as jnp

D = 8192
FF_WIN = 2048
TOKENS = 2048


def spiked(values, stream_key, source, target, blocks, factor):
    def block_of(dim):
        return (jnp.arange(values.shape[dim]) // (values.shape[dim] // blocks)).reshape((-1,) + (1,) * (values.ndim - 1 - dim))

    one_side = jax.random.permutation(stream_key, blocks)[block_of(target)]
    other_side = (block_of(target) + blocks // 2) % blocks
    return jnp.where((block_of(source) == one_side) | (block_of(source) == other_side), factor * values, values)


def level_of(key, dims, shards, low, largest):
    factor_of = 1.0
    for dim, shards_of in shards:
        heights = jax.random.uniform(jax.random.fold_in(jax.random.fold_in(key, 6), dim), (shards_of,), jnp.float32, low / len(shards), largest / len(shards))
        factor_of = factor_of * jnp.repeat(jnp.exp(heights), dims[dim] // shards_of).reshape((-1,) + (1,) * (len(dims) - 1 - dim))
    return factor_of


def gaussian(key, extent, deviation, bound, pieces=(), dtype=jnp.bfloat16):
    array = jax.random.normal(key, extent, jnp.float32) * deviation
    if len(pieces) > 0:
        array = level_of(key, extent, pieces, -0.22, 0.18) * array
    return jnp.clip(array, min=-bound, max=bound).astype(dtype)


def bell_draw_with(rng, shape, width, most, split, heavy, kind=jnp.bfloat16):
    result = width * jax.random.normal(rng, shape, jnp.float32)
    if split:
        result = result * level_of(rng, shape, split, -0.22, 0.18)
    return jnp.clip(spiked(result, jax.random.fold_in(rng, 3), *heavy), -most, most).astype(kind)


def setup_inputs(seed: int = 0) -> dict:
    seeds = jax.random.split(jax.random.key(seed), 6)
    return {
        "tokens": bell_draw_with(seeds[0], (TOKENS, D), 1.0, 6.0, ((0, 8), (1, 16)), (0, 1, 16, 2.0)),
        "out_grad": bell_draw_with(seeds[1], (TOKENS, D), 1.0, 6.0, ((0, 8), (1, 16)), (0, 1, 16, 2.0)),
        "gate_weight": gaussian(seeds[2], (D, FF_WIN), D ** -0.5, 0.0625, ((0, 8), (1, 16))),
        "up_weight": gaussian(seeds[3], (D, FF_WIN), D ** -0.5, 0.0625, ((0, 8), (1, 16))),
        "down_weight": gaussian(seeds[4], (FF_WIN, D), FF_WIN ** -0.5, 0.125, ((0, 16), (1, 8))),
    }


def reference(tokens, out_grad, gate_weight, up_weight, down_weight):
    gate = jnp.dot(tokens, gate_weight, preferred_element_type=jnp.float32)
    up = jnp.dot(tokens, up_weight, preferred_element_type=jnp.float32)
    squashed = jax.nn.sigmoid(gate)
    activated = gate * squashed
    slope = squashed * (1.0 + gate * (1.0 - squashed))
    hidden = (activated * up).astype(jnp.bfloat16)
    hidden_grad = jnp.dot(out_grad, down_weight.T, preferred_element_type=jnp.float32)
    gate_delta = (hidden_grad * up * slope).astype(jnp.bfloat16)
    up_delta = (hidden_grad * activated).astype(jnp.bfloat16)
    input_grad = jnp.dot(gate_delta, gate_weight.T, preferred_element_type=jnp.float32)
    input_grad = input_grad + jnp.dot(up_delta, up_weight.T, preferred_element_type=jnp.float32)
    factor = 1.0 / math.sqrt(TOKENS)
    gate_grad = jnp.dot(tokens.T, gate_delta, preferred_element_type=jnp.float32) * factor
    up_grad = jnp.dot(tokens.T, up_delta, preferred_element_type=jnp.float32) * factor
    down_grad = jnp.dot(hidden.T, out_grad, preferred_element_type=jnp.float32) * factor
    return (input_grad.astype(jnp.bfloat16), gate_grad, up_grad, down_grad)
```

```python
import math

import jax
import jax.numpy as jnp
from jax import lax
from jax.sharding import Mesh
from jax.sharding import PartitionSpec as P

AXES = ("zh", "y", "zl", "x", "c")
SIZES = (2, 4, 2, 4, 2)
BF16 = jnp.bfloat16
F32 = jnp.float32


def number(place):
    at = 0
    for size, coordinate in zip(SIZES, place):
        at = at * size + coordinate
    return at


def places():
    found = [()]
    for size in SIZES:
        found = [(*place, k) for place in found for k in range(size)]
    return found


def moved(value, target):
    pairs = [(number(p), number(target(*p))) for p in places()]
    return lax.ppermute(value, AXES, pairs)


def moved_back(value, target):
    pairs = [(number(target(*p)), number(p)) for p in places()]
    return lax.ppermute(value, AXES, pairs)


def turned(value, axis, step):
    return lax.ppermute(value, axis, [(i, (i + step) % 4) for i in range(4)])


def other_core(value):
    return lax.ppermute(value, "c", [(0, 1), (1, 0)])


def stay(zh, y, zl, x, c):
    return (zh, x, zl, (x - y) % 4, c)


def cross(zh, y, zl, x, c):
    return (zh, x, 1 - zl, (x - y) % 4, c)


def along_z(value, mask):
    return moved(value, lambda zh, y, zl, x, c: (zh ^ (mask >> 1), y, zl ^ (mask & 1), x, c))


def swapped(flag, first, second):
    return jnp.where(flag, second, first), jnp.where(flag, first, second)


def dot(a, b, da, db):
    return lax.dot_general(a, b, (((da,), (db,)), ((), ())), preferred_element_type=F32)


def shards(tokens, out_grad, gate_weight, up_weight, down_weight):
    factor = 1.0 / math.sqrt(tokens.shape[0] * 8)
    zh, zl, c = lax.axis_index("zh"), lax.axis_index("zl"), lax.axis_index("c")
    half = tokens.shape[0] // 2
    deep = gate_weight.shape[0] // 2
    units = gate_weight.shape[1]
    uneven = zh != zl

    def to_blocks(value):
        mine = lax.dynamic_slice_in_dim(value, zl * half, half, 0)
        theirs = lax.dynamic_slice_in_dim(value, (1 - zl) * half, half, 0)
        pieces = swapped(uneven, moved(mine, stay), moved(theirs, cross))
        return jnp.concatenate(pieces, axis=1)

    def over_x(block):
        rows = [block] + [turned(block, "x", k) for k in (1, 2, 3)]
        own = jnp.concatenate(rows, axis=0)
        return jnp.concatenate([own, other_core(own)], axis=1)

    def halves(value, dim):
        a = lax.slice_in_dim(value, 0, deep, axis=dim)
        b = lax.slice_in_dim(value, deep, 2 * deep, axis=dim)
        return swapped(c == 1, a, b)

    gu = jnp.concatenate([gate_weight, up_weight], axis=1)
    gus = [gu] + [along_z(gu, m) for m in (1, 2, 3)]
    downs = [down_weight] + [along_z(down_weight, m) for m in (1, 2, 3)]
    gu_rows, down_columns = [], []
    for core in (0, 1):
        for a in (0, 1):
            left, right = halves(gus[2 * a], 0)[core], halves(gus[2 * a + 1], 0)[core]
            gu_rows.append(
                jnp.concatenate([left[:, :units], right[:, :units], left[:, units:], right[:, units:]], axis=1)
            )
            down_columns.append(
                jnp.concatenate([halves(downs[2 * a], 1)[core], halves(downs[2 * a + 1], 1)[core]], axis=0)
            )
    gu_full = jnp.concatenate(gu_rows, axis=0)
    down_full = jnp.concatenate(down_columns, axis=1)

    x_block = to_blocks(tokens)
    g_block = to_blocks(out_grad)
    x_full = over_x(x_block)
    g_full = over_x(g_block)

    def summed_over_y(part):
        total = part[:half]
        for k in (1, 2, 3):
            total = total + turned(part[k * half : (k + 1) * half], "y", k)
        return total

    width = 2 * units
    gate_up = summed_over_y(dot(x_full, gu_full, 1, 0))
    hidden_grad = summed_over_y(dot(g_full, down_full, 1, 1))
    gate, up = gate_up[:, :width], gate_up[:, width:]
    squashed = jax.nn.sigmoid(gate)
    activated = gate * squashed
    slope = squashed * (1.0 + gate * (1.0 - squashed))
    hidden = (activated * up).astype(BF16)
    gate_delta = (hidden_grad * up * slope).astype(BF16)
    up_delta = (hidden_grad * activated).astype(BF16)
    deltas = jnp.concatenate([gate_delta, up_delta], axis=1)

    def over_y(block):
        rows = [block] + [turned(block, "y", k) for k in (1, 2, 3)]
        return jnp.concatenate([rows[0], rows[3], rows[2], rows[1]], axis=0)

    hidden_all = over_y(hidden)
    deltas_all = over_y(deltas)

    parts = dot(deltas_all, gu_full, 1, 1)
    mine, theirs = parts[:, : 2 * deep], parts[:, 2 * deep :]
    parts = mine + other_core(theirs)
    total = parts[:half]
    for j in (1, 2, 3):
        total = total + turned(parts[j * half : (j + 1) * half], "x", -j)
    total = total.astype(BF16)
    kept, sent = swapped(uneven, total[:, :deep], total[:, deep:])
    input_grad = jnp.concatenate(swapped(zl == 1, moved_back(kept, stay), moved_back(sent, cross)), axis=0)

    gu_part = dot(x_full, deltas_all, 0, 0) * factor
    down_part = dot(hidden_all, g_full, 0, 0) * factor

    def gu_piece(mask, which):
        a, b = mask >> 1, mask & 1
        at = which * width + b * units
        return jnp.concatenate(
            [gu_part[(2 * core + a) * deep : (2 * core + a + 1) * deep, at : at + units] for core in (0, 1)], axis=0
        )

    def down_piece(mask):
        a, b = mask >> 1, mask & 1
        rows = down_part[b * units : (b + 1) * units]
        return jnp.concatenate(
            [rows[:, (2 * core + a) * deep : (2 * core + a + 1) * deep] for core in (0, 1)], axis=1
        )

    def summed_over_z(piece, dim):
        total = piece(0)
        for m in (1, 2, 3):
            total = total + along_z(piece(m).astype(BF16), m).astype(F32)
        return jnp.concatenate(halves(total, dim), axis=dim)

    gate_grad = summed_over_z(lambda m: gu_piece(m, 0), 0)
    up_grad = summed_over_z(lambda m: gu_piece(m, 1), 0)
    down_grad = summed_over_z(down_piece, 1)
    return (input_grad, gate_grad, up_grad, down_grad)


def solution(mesh):
    finer = Mesh(mesh.devices.reshape(SIZES), AXES)
    rows, columns = ("zh", "y"), ("zl", "x", "c")
    return jax.shard_map(
        shards,
        mesh=finer,
        in_specs=(P(rows, columns),) * 4 + (P(columns, rows),),
        out_specs=(P(rows, columns),) * 3 + (P(columns, rows),),
        check_vma=False,
    )
```

```python
import functools
import math

import jax
import jax.numpy as jnp
from jax import lax
from jax.experimental import pallas as pl
from jax.experimental.pallas import tpu as pltpu
from jax.sharding import Mesh
from jax.sharding import PartitionSpec as P

AXES = ("zh", "y", "zl", "x", "c")
SIZES = (2, 4, 2, 4, 2)
BF16 = jnp.bfloat16
F32 = jnp.float32
STEPS = (1, 3, 2)
F16 = jnp.float16
TOP = 14.0
NOTE = 16


def number(place):
    at = 0
    for size, coordinate in zip(SIZES, place):
        at = at * size + coordinate
    return at


def places():
    found = [()]
    for size in SIZES:
        found = [(*place, k) for place in found for k in range(size)]
    return found


def moved(value, target, back=False):
    pairs = [(number(p), number(target(*p))) for p in places()]
    if back:
        pairs = [(b, a) for a, b in pairs]
    return lax.ppermute(value, AXES, pairs)


def turned(value, axis, step):
    return lax.ppermute(value, axis, [(i, (i + step) % 4) for i in range(4)])


def other_core(value):
    return lax.ppermute(value, "c", [(0, 1), (1, 0)])


def stay(zh, y, zl, x, c):
    return (zh, x, zl, (x - y) % 4, c)


def cross(zh, y, zl, x, c):
    return (zh, x, 1 - zl, (x - y) % 4, c)


def along_z(value, mask):
    return moved(value, lambda zh, y, zl, x, c: (zh ^ (mask >> 1), y, zl ^ (mask & 1), x, c))


def call(body, scalars, arrays, outs, flops):
    smem = pl.BlockSpec(memory_space=pltpu.SMEM)
    vmem = pl.BlockSpec(memory_space=pltpu.VMEM)
    return pl.pallas_call(
        body,
        in_specs=[smem] * len(scalars) + [vmem] * len(arrays),
        out_specs=[vmem] * len(outs),
        out_shape=[jax.ShapeDtypeStruct(s, t) for s, t in outs],
        compiler_params=pltpu.CompilerParams(vmem_limit_bytes=8 * 1024 * 1024),
        cost_estimate=pl.CostEstimate(flops=flops, bytes_accessed=1 << 20, transcendentals=0),
    )(*scalars, *arrays)


def dot(a, b, da, db):
    return lax.dot_general(a, b, (((da,), (db,)), ((), ())), preferred_element_type=F32)


def pack_kernel(flag_ref, p_ref, q_ref, out_ref):
    wide = p_ref.shape[1]

    @pl.when(flag_ref[0] == 0)
    def _():
        out_ref[:, :wide] = p_ref[...]
        out_ref[:, wide:] = q_ref[...]

    @pl.when(flag_ref[0] != 0)
    def _():
        out_ref[:, :wide] = q_ref[...]
        out_ref[:, wide:] = p_ref[...]


def join_kernel(a_ref, b_ref, out_ref):
    wide = a_ref.shape[1]
    out_ref[:, :wide] = a_ref[...]
    out_ref[:, wide:] = b_ref[...]


def stacked(refs, at):
    return jnp.concatenate([r[:, at] for r in refs], axis=0)


def put_parts(outs, pieces, half):
    largest = None
    for _, value in pieces:
        size = jnp.max(jnp.abs(value), axis=(0, 1), keepdims=True)
        largest = size if largest is None else jnp.maximum(largest, size)
    exponent = jnp.clip(jnp.floor(jnp.log2(largest)), -100.0, 100.0)
    scale = jnp.exp2(TOP - exponent)
    for at, value in pieces:
        outs[0][:, at] = value[:half]
        for k in (1, 2, 3):
            outs[k][:half, at] = value[k * half : (k + 1) * half] * scale
    for k in (1, 2, 3):
        outs[k][half:, :] = jnp.broadcast_to(exponent, (NOTE, outs[k].shape[1]))


def forward_kernel(core_ref, *refs, transposed, kinds):
    own, other, weights, outs = refs[:4], refs[4:8], refs[8:12], refs[12:16]
    core = core_ref[0]
    half = own[0].shape[0]
    deep = own[0].shape[1] // 2
    totals = [None, None]
    for side, rows in ((core, own), (1 - core, other)):
        at = pl.ds(pl.multiple_of(side * deep, deep), deep)
        for a in (0, 1):
            block = stacked(rows, slice(a * deep, (a + 1) * deep))
            for b in (0, 1):
                if transposed:
                    term = dot(block, weights[2 * a + b][:, at], 1, 1)
                else:
                    term = dot(block, weights[2 * a + b][at, :], 1, 0)
                totals[b] = term if totals[b] is None else totals[b] + term
    units = totals[0].shape[1] // kinds
    pieces = []
    for b in (0, 1):
        for kind in range(kinds):
            place = (2 * kind + b) * units
            pieces.append((slice(place, place + units), totals[b][:, kind * units : (kind + 1) * units]))
    put_parts(outs, pieces, half)


def activation_kernel(sum_ref, hidden_ref, slope_ref, activated_ref):
    width = hidden_ref.shape[1]
    gate, up = sum_ref[:, :width], sum_ref[:, width:]
    squashed = jax.nn.sigmoid(gate)
    activated = gate * squashed
    hidden_ref[...] = (activated * up).astype(BF16)
    slope_ref[...] = up * (squashed * (1.0 + gate * (1.0 - squashed)))
    activated_ref[...] = activated


def delta_kernel(grad_ref, slope_ref, activated_ref, out_ref):
    width = grad_ref.shape[1]
    out_ref[:, :width] = (grad_ref[...] * slope_ref[...]).astype(BF16)
    out_ref[:, width:] = (grad_ref[...] * activated_ref[...]).astype(BF16)


def delta_columns(refs, b):
    units = refs[0].shape[1] // 4
    return jnp.concatenate(
        [stacked(refs, slice((2 * kind + b) * units, (2 * kind + b + 1) * units)) for kind in (0, 1)], axis=1
    )


def down_grad_kernel(core_ref, *refs, factor):
    hidden, own, other, outs = refs[:4], refs[4:8], refs[8:12], refs[12:16]
    core = core_ref[0]
    deep = own[0].shape[1] // 2
    units = hidden[0].shape[1] // 2
    left = stacked(hidden, slice(None))
    for side, rows in ((core, own), (1 - core, other)):
        at = pl.ds(pl.multiple_of(side * deep, deep), deep)
        for a in (0, 1):
            total = dot(left, stacked(rows, slice(a * deep, (a + 1) * deep)), 0, 0)
            for b in (0, 1):
                out = outs[2 * a + b]
                out[:, at] = (total[b * units : (b + 1) * units] * factor).astype(out.dtype)


def gate_up_grad_kernel(core_ref, *refs, factor):
    deltas, own, other, outs = refs[:4], refs[4:8], refs[8:12], refs[12:16]
    core = core_ref[0]
    deep = own[0].shape[1] // 2
    right = [delta_columns(deltas, b) for b in (0, 1)]
    for side, rows in ((core, own), (1 - core, other)):
        at = pl.ds(pl.multiple_of(side * deep, deep), deep)
        for a in (0, 1):
            left = stacked(rows, slice(a * deep, (a + 1) * deep))
            for b in (0, 1):
                out = outs[2 * a + b]
                out[at, :] = (dot(left, right[b], 0, 0) * factor).astype(out.dtype)


def input_grad_kernel(core_ref, *refs):
    deltas, weights, outs = (refs[:4], refs[4:8]), (refs[8:12], refs[12:16]), refs[16:20]
    half = deltas[0][0].shape[0]
    deep = weights[0][0].shape[0] // 2
    at = pl.ds(pl.multiple_of(core_ref[0] * deep, deep), deep)
    left = [[delta_columns(deltas[side], b) for b in (0, 1)] for side in (0, 1)]
    pieces = []
    for a in (0, 1):
        total = None
        for side in (0, 1):
            for b in (0, 1):
                term = dot(left[side][b], weights[side][2 * a + b][at, :], 1, 1)
                total = term if total is None else total + term
        pieces.append((slice(a * deep, (a + 1) * deep), total))
    put_parts(outs, pieces, half)


def step(tokens, out_grad, gate_weight, up_weight, down_weight):
    factor = 1.0 / math.sqrt(tokens.shape[0] * 8)
    zh, zl, c = lax.axis_index("zh"), lax.axis_index("zl"), lax.axis_index("c")
    half = tokens.shape[0] // 2
    deep = gate_weight.shape[0] // 2
    units = gate_weight.shape[1]
    width = 2 * units
    uneven = (zh ^ zl).reshape(1)
    core = c.reshape(1)
    wide = 2 * deep

    def to_block(value):
        mine = lax.dynamic_slice_in_dim(value, zl * half, half, 0)
        theirs = lax.dynamic_slice_in_dim(value, (1 - zl) * half, half, 0)
        p, q = moved(mine, stay), moved(theirs, cross)
        return call(pack_kernel, [uneven], [p, q], [((half, wide), tokens.dtype)], 1000)[0]

    def over_x(block):
        rows = {0: block}
        for k in STEPS:
            rows[k] = turned(block, "x", k)
        other = {k: other_core(rows[k]) for k in (0, *STEPS)}
        return [rows[k] for k in range(4)], [other[k] for k in range(4)]

    def pieces(value):
        found = {0: value}
        for m in STEPS:
            found[m] = along_z(value, m)
        return [found[m] for m in range(4)]

    x_own, x_other = over_x(to_block(tokens))
    g_own, g_other = over_x(to_block(out_grad))
    joined = call(join_kernel, [], [gate_weight, up_weight], [((wide, width), BF16)], 1000)[0]
    gu = pieces(joined)
    down = pieces(down_weight)

    gu_other = [other_core(gu[m]) for m in range(4)]

    def parts_of(columns):
        return [((half, columns), F32)] + [((half + NOTE, columns), F32)] * 3

    gu_flops = 2 * 4 * half * 4 * deep * 2 * width
    gu_parts = call(
        functools.partial(forward_kernel, transposed=False, kinds=2), [core],
        [*x_own, *x_other, *gu], parts_of(2 * width), gu_flops,
    )
    down_parts = call(
        functools.partial(forward_kernel, transposed=True, kinds=1), [core],
        [*g_own, *g_other, *down], parts_of(width), gu_flops // 2,
    )

    def summed(parts, axis):
        total = parts[0]
        sent = [p.astype(F16) for p in parts]
        for k in STEPS:
            got = turned(sent[k], axis, k).astype(F32)
            total = total + got[:half] * jnp.exp2(got[half : half + 1] - TOP)
        return total

    gate_up = summed(gu_parts, "y")
    hidden_grad = summed(down_parts, "y")
    hidden, slope, activated = call(
        activation_kernel, [], [gate_up],
        [((half, width), BF16), ((half, width), F32), ((half, width), F32)], 1000,
    )
    deltas = call(delta_kernel, [], [hidden_grad, slope, activated], [((half, 2 * width), BF16)], 1000)[0]

    def over_y(block):
        rows = {0: block}
        for k in STEPS:
            rows[k] = turned(block, "y", k)
        return [rows[k] for k in range(4)]

    hidden_rows = over_y(hidden)
    delta_rows = over_y(deltas)
    delta_other = [other_core(delta_rows[k]) for k in range(4)]

    def matching(rows):
        return [rows[0], rows[3], rows[2], rows[1]]

    down_out = call(
        functools.partial(down_grad_kernel, factor=factor), [core],
        [*matching(hidden_rows), *g_own, *g_other],
        [((units, wide), F32)] + [((units, wide), BF16)] * 3, gu_flops // 2,
    )
    ig_parts = call(
        input_grad_kernel, [core], [*delta_rows, *delta_other, *gu, *gu_other],
        parts_of(wide), gu_flops,
    )
    gu_out = call(
        functools.partial(gate_up_grad_kernel, factor=factor), [core],
        [*matching(delta_rows), *x_own, *x_other],
        [((wide, width), F32)] + [((wide, width), BF16)] * 3, gu_flops,
    )

    def from_z(outs):
        return [outs[0]] + [along_z(outs[m], m) for m in STEPS]

    def total_of(terms, at):
        total = terms[0][:, at]
        for term in terms[1:]:
            total = total + term[:, at].astype(F32)
        return total

    down_grad = total_of(from_z(down_out), slice(None))
    gu_terms = from_z(gu_out)
    gate_grad, up_grad = total_of(gu_terms, slice(0, units)), total_of(gu_terms, slice(units, width))

    total = summed(ig_parts, "x").astype(BF16)
    kept = jnp.where(zh == zl, total[:, :deep], total[:, deep:])
    sent = jnp.where(zh == zl, total[:, deep:], total[:, :deep])
    kept, sent = moved(kept, stay, back=True), moved(sent, cross, back=True)
    input_grad = jnp.concatenate([jnp.where(zl == 0, kept, sent), jnp.where(zl == 0, sent, kept)], axis=0)
    return (input_grad, gate_grad, up_grad, down_grad)


def solution(mesh):
    finer = Mesh(mesh.devices.reshape(SIZES), AXES)
    rows, columns = ("zh", "y"), ("zl", "x", "c")
    return jax.shard_map(
        step,
        mesh=finer,
        in_specs=(P(rows, columns),) * 4 + (P(columns, rows),),
        out_specs=(P(rows, columns),) * 3 + (P(columns, rows),),
        check_vma=False,
    )
```

```python
import functools
import math

import jax
import jax.numpy as jnp
from jax import lax
from jax.experimental import pallas as pl
from jax.experimental.pallas import tpu as pltpu
from jax.sharding import Mesh
from jax.sharding import PartitionSpec as P

AXES = ("zh", "y", "zl", "x", "c")
SIZES = (2, 4, 2, 4, 2)
BF16 = jnp.bfloat16
F32 = jnp.float32
STEPS = (1, 3, 2)
F16 = jnp.float16
TOP = 14.0
NOTE = 16


def number(place):
    at = 0
    for size, coordinate in zip(SIZES, place):
        at = at * size + coordinate
    return at


def places():
    found = [()]
    for size in SIZES:
        found = [(*place, k) for place in found for k in range(size)]
    return found


def moved(value, target, back=False):
    pairs = [(number(p), number(target(*p))) for p in places()]
    if back:
        pairs = [(b, a) for a, b in pairs]
    return lax.ppermute(value, AXES, pairs)


def turned(value, axis, step):
    return lax.ppermute(value, axis, [(i, (i + step) % 4) for i in range(4)])


def other_core(value):
    return lax.ppermute(value, "c", [(0, 1), (1, 0)])


def stay(zh, y, zl, x, c):
    return (zh, x, zl, (x - y) % 4, c)


def cross(zh, y, zl, x, c):
    return (zh, x, 1 - zl, (x - y) % 4, c)


def along_z(value, mask):
    return moved(value, lambda zh, y, zl, x, c: (zh ^ (mask >> 1), y, zl ^ (mask & 1), x, c))


def call(body, scalars, arrays, outs, flops):
    smem = pl.BlockSpec(memory_space=pltpu.SMEM)
    vmem = pl.BlockSpec(memory_space=pltpu.VMEM)
    return pl.pallas_call(
        body,
        in_specs=[smem] * len(scalars) + [vmem] * len(arrays),
        out_specs=[vmem] * len(outs),
        out_shape=[jax.ShapeDtypeStruct(s, t) for s, t in outs],
        compiler_params=pltpu.CompilerParams(vmem_limit_bytes=8 * 1024 * 1024),
        cost_estimate=pl.CostEstimate(flops=flops, bytes_accessed=1 << 20, transcendentals=0),
    )(*scalars, *arrays)


def dot(a, b, da, db):
    return lax.dot_general(a, b, (((da,), (db,)), ((), ())), preferred_element_type=F32)


CORE, UNEVEN, LOW = 0, 1, 2


def ordered_copy(swap, first, second, left, right):
    @pl.when(swap == 0)
    def _():
        left[...] = first[...]
        right[...] = second[...]

    @pl.when(swap != 0)
    def _():
        left[...] = second[...]
        right[...] = first[...]


def pack_kernel(flags, p_ref, q_ref, out_ref):
    wide = p_ref.shape[1]
    ordered_copy(flags[UNEVEN], p_ref, q_ref, out_ref.at[:, :wide], out_ref.at[:, wide:])


def unpack_kernel(flags, in_ref, kept_ref, sent_ref):
    wide = kept_ref.shape[1]
    ordered_copy(flags[UNEVEN], in_ref.at[:, :wide], in_ref.at[:, wide:], kept_ref, sent_ref)


def merge_kernel(flags, kept_ref, sent_ref, out_ref):
    rows = kept_ref.shape[0]
    ordered_copy(flags[LOW], kept_ref, sent_ref, out_ref.at[:rows], out_ref.at[rows:])


def join_kernel(a_ref, b_ref, out_ref):
    wide = a_ref.shape[1]
    out_ref[:, :wide] = a_ref[...]
    out_ref[:, wide:] = b_ref[...]


def stacked(refs, at):
    return jnp.concatenate([r[:, at] for r in refs], axis=0)


def put_parts(outs, pieces, half):
    largest = None
    for _, value in pieces:
        size = jnp.max(jnp.abs(value), axis=(0, 1), keepdims=True)
        largest = size if largest is None else jnp.maximum(largest, size)
    exponent = jnp.clip(jnp.floor(jnp.log2(largest)), -100.0, 100.0)
    scale = jnp.exp2(TOP - exponent)
    for at, value in pieces:
        outs[0][:, at] = value[:half]
        for k in (1, 2, 3):
            outs[k][:half, at] = value[k * half : (k + 1) * half] * scale
    for k in (1, 2, 3):
        outs[k][half:, :] = jnp.broadcast_to(exponent, (NOTE, outs[k].shape[1]))


def forward_kernel(core_ref, *refs, transposed, kinds):
    own, other, weights, outs = refs[:4], refs[4:8], refs[8:12], refs[12:16]
    core = core_ref[CORE]
    half = own[0].shape[0]
    deep = own[0].shape[1] // 2
    totals = [None, None]
    for side, rows in ((core, own), (1 - core, other)):
        at = pl.ds(pl.multiple_of(side * deep, deep), deep)
        for a in (0, 1):
            block = stacked(rows, slice(a * deep, (a + 1) * deep))
            for b in (0, 1):
                if transposed:
                    term = dot(block, weights[2 * a + b][:, at], 1, 1)
                else:
                    term = dot(block, weights[2 * a + b][at, :], 1, 0)
                totals[b] = term if totals[b] is None else totals[b] + term
    units = totals[0].shape[1] // kinds
    pieces = []
    for b in (0, 1):
        for kind in range(kinds):
            place = (2 * kind + b) * units
            pieces.append((slice(place, place + units), totals[b][:, kind * units : (kind + 1) * units]))
    put_parts(outs, pieces, half)


def activation_kernel(sum_ref, hidden_ref, slope_ref, activated_ref):
    width = hidden_ref.shape[1]
    gate, up = sum_ref[:, :width], sum_ref[:, width:]
    squashed = jax.nn.sigmoid(gate)
    activated = gate * squashed
    hidden_ref[...] = (activated * up).astype(BF16)
    slope_ref[...] = up * (squashed * (1.0 + gate * (1.0 - squashed)))
    activated_ref[...] = activated


def delta_kernel(grad_ref, slope_ref, activated_ref, out_ref):
    width = grad_ref.shape[1]
    out_ref[:, :width] = (grad_ref[...] * slope_ref[...]).astype(BF16)
    out_ref[:, width:] = (grad_ref[...] * activated_ref[...]).astype(BF16)


def delta_columns(refs, b):
    units = refs[0].shape[1] // 4
    return jnp.concatenate(
        [stacked(refs, slice((2 * kind + b) * units, (2 * kind + b + 1) * units)) for kind in (0, 1)], axis=1
    )


def down_grad_kernel(core_ref, *refs, factor):
    hidden, own, other, outs = refs[:4], refs[4:8], refs[8:12], refs[12:16]
    core = core_ref[CORE]
    deep = own[0].shape[1] // 2
    units = hidden[0].shape[1] // 2
    left = stacked(hidden, slice(None))
    for side, rows in ((core, own), (1 - core, other)):
        at = pl.ds(pl.multiple_of(side * deep, deep), deep)
        for a in (0, 1):
            total = dot(left, stacked(rows, slice(a * deep, (a + 1) * deep)), 0, 0)
            for b in (0, 1):
                out = outs[2 * a + b]
                out[:, at] = (total[b * units : (b + 1) * units] * factor).astype(out.dtype)


def gate_up_grad_kernel(core_ref, *refs, factor):
    deltas, own, other, outs = refs[:4], refs[4:8], refs[8:12], refs[12:16]
    core = core_ref[CORE]
    deep = own[0].shape[1] // 2
    right = [delta_columns(deltas, b) for b in (0, 1)]
    for side, rows in ((core, own), (1 - core, other)):
        at = pl.ds(pl.multiple_of(side * deep, deep), deep)
        for a in (0, 1):
            left = stacked(rows, slice(a * deep, (a + 1) * deep))
            for b in (0, 1):
                out = outs[2 * a + b]
                out[at, :] = (dot(left, right[b], 0, 0) * factor).astype(out.dtype)


def input_grad_kernel(core_ref, *refs):
    deltas, weights, outs = (refs[:4], refs[4:8]), (refs[8:12], refs[12:16]), refs[16:20]
    half = deltas[0][0].shape[0]
    deep = weights[0][0].shape[0] // 2
    at = pl.ds(pl.multiple_of(core_ref[CORE] * deep, deep), deep)
    left = [[delta_columns(deltas[side], b) for b in (0, 1)] for side in (0, 1)]
    pieces = []
    for a in (0, 1):
        total = None
        for side in (0, 1):
            for b in (0, 1):
                term = dot(left[side][b], weights[side][2 * a + b][at, :], 1, 1)
                total = term if total is None else total + term
        pieces.append((slice(a * deep, (a + 1) * deep), total))
    put_parts(outs, pieces, half)


def step(tokens, out_grad, gate_weight, up_weight, down_weight):
    factor = 1.0 / math.sqrt(tokens.shape[0] * 8)
    zh, zl, c = lax.axis_index("zh"), lax.axis_index("zl"), lax.axis_index("c")
    half = tokens.shape[0] // 2
    deep = gate_weight.shape[0] // 2
    units = gate_weight.shape[1]
    width = 2 * units
    wide = 2 * deep
    flags = jnp.stack([c, zh ^ zl, zl]).astype(jnp.int32)

    def to_block(value):
        mine = lax.dynamic_slice_in_dim(value, zl * half, half, 0)
        theirs = lax.dynamic_slice_in_dim(value, (1 - zl) * half, half, 0)
        p, q = moved(mine, stay), moved(theirs, cross)
        return call(pack_kernel, [flags], [p, q], [((half, wide), tokens.dtype)], 1000)[0]

    def over_x(block):
        rows = {0: block}
        for k in STEPS:
            rows[k] = turned(block, "x", k)
        other = {k: other_core(rows[k]) for k in (0, *STEPS)}
        return [rows[k] for k in range(4)], [other[k] for k in range(4)]

    def pieces(value):
        found = {0: value}
        for m in STEPS:
            found[m] = along_z(value, m)
        return [found[m] for m in range(4)]

    x_own, x_other = over_x(to_block(tokens))
    g_own, g_other = over_x(to_block(out_grad))
    joined = call(join_kernel, [], [gate_weight, up_weight], [((wide, width), BF16)], 1000)[0]
    gu = pieces(joined)
    down = pieces(down_weight)

    gu_other = [other_core(gu[m]) for m in range(4)]

    def parts_of(columns):
        return [((half, columns), F32)] + [((half + NOTE, columns), F32)] * 3

    gu_flops = 2 * 4 * half * 4 * deep * 2 * width
    gu_parts = call(
        functools.partial(forward_kernel, transposed=False, kinds=2), [flags],
        [*x_own, *x_other, *gu], parts_of(2 * width), gu_flops,
    )
    down_parts = call(
        functools.partial(forward_kernel, transposed=True, kinds=1), [flags],
        [*g_own, *g_other, *down], parts_of(width), gu_flops // 2,
    )

    def summed(parts, axis):
        total = parts[0]
        sent = [p.astype(F16) for p in parts]
        for k in STEPS:
            got = turned(sent[k], axis, k).astype(F32)
            total = total + got[:half] * jnp.exp2(got[half : half + 1] - TOP)
        return total

    gate_up = summed(gu_parts, "y")
    hidden_grad = summed(down_parts, "y")
    hidden, slope, activated = call(
        activation_kernel, [], [gate_up],
        [((half, width), BF16), ((half, width), F32), ((half, width), F32)], 1000,
    )
    deltas = call(delta_kernel, [], [hidden_grad, slope, activated], [((half, 2 * width), BF16)], 1000)[0]

    def over_y(block):
        rows = {0: block}
        for k in STEPS:
            rows[k] = turned(block, "y", k)
        return [rows[k] for k in range(4)]

    hidden_rows = over_y(hidden)
    delta_rows = over_y(deltas)
    delta_other = [other_core(delta_rows[k]) for k in range(4)]

    def matching(rows):
        return [rows[0], rows[3], rows[2], rows[1]]

    down_out = call(
        functools.partial(down_grad_kernel, factor=factor), [flags],
        [*matching(hidden_rows), *g_own, *g_other],
        [((units, wide), F32)] + [((units, wide), BF16)] * 3, gu_flops // 2,
    )
    ig_parts = call(
        input_grad_kernel, [flags], [*delta_rows, *delta_other, *gu, *gu_other],
        parts_of(wide), gu_flops,
    )
    gu_out = call(
        functools.partial(gate_up_grad_kernel, factor=factor), [flags],
        [*matching(delta_rows), *x_own, *x_other],
        [((wide, width), F32)] + [((wide, width), BF16)] * 3, gu_flops,
    )

    def from_z(outs):
        return [outs[0]] + [along_z(outs[m], m) for m in STEPS]

    def total_of(terms, at):
        total = terms[0][:, at]
        for term in terms[1:]:
            total = total + term[:, at].astype(F32)
        return total

    down_grad = total_of(from_z(down_out), slice(None))
    gu_terms = from_z(gu_out)
    gate_grad, up_grad = total_of(gu_terms, slice(0, units)), total_of(gu_terms, slice(units, width))

    total = summed(ig_parts, "x").astype(BF16)
    kept, sent = call(unpack_kernel, [flags], [total], [((half, deep), BF16)] * 2, 1000)
    kept, sent = moved(kept, stay, back=True), moved(sent, cross, back=True)
    input_grad = call(merge_kernel, [flags], [kept, sent], [((2 * half, deep), BF16)], 1000)[0]
    return (input_grad, gate_grad, up_grad, down_grad)


def solution(mesh):
    finer = Mesh(mesh.devices.reshape(SIZES), AXES)
    rows, columns = ("zh", "y"), ("zl", "x", "c")
    return jax.shard_map(
        step,
        mesh=finer,
        in_specs=(P(rows, columns),) * 4 + (P(columns, rows),),
        out_specs=(P(rows, columns),) * 3 + (P(columns, rows),),
        check_vma=False,
    )
```
